32 devices in a mesh: dp: 4 (over y, z), tp: 8 (over x, core).
Axes of the slice: x: 4, y: 2, z: 2, core: 2. Of those that a mesh axis runs over, the one named last changes fastest.
The devices are a block of a 4x4x8 slice.
Arguments:
- hidden: bfloat16 [128, 1536], P('dp'), parts along dimension 0
- lengths: int32 [128], P('dp'), parts along dimension 0
- choice: int32 [2, 128, 8], P(None, 'dp'), parts along dimension 1
- keys_one: bfloat16 [128, 128, 8, 64], P('dp', 'tp'), parts along dimension 0
- vals_one: bfloat16 [128, 128, 8, 64], P('dp', 'tp'), parts along dimension 0
- keys_two: bfloat16 [128, 128, 8, 64], P('dp', 'tp'), parts along dimension 0
- vals_two: bfloat16 [128, 128, 8, 64], P('dp', 'tp'), parts along dimension 0
- g_attn: bfloat16 [2, 1536], replicated
- w_q: bfloat16 [2, 1536, 1536], P(None, None, 'tp')
- w_k: bfloat16 [2, 1536, 512], P(None, None, 'tp')
- w_v: bfloat16 [2, 1536, 512], P(None, None, 'tp')
- w_o: bfloat16 [2, 1536, 1536], P(None, 'tp')
- g_mlp: bfloat16 [2, 1536], replicated
- w_router: bfloat16 [2, 1536, 40], replicated
- w_gate: bfloat16 [2, 40, 1536, 512], P(None, None, None, 'tp')
- w_up: bfloat16 [2, 40, 1536, 512], P(None, None, None, 'tp')
- w_down: bfloat16 [2, 40, 512, 1536], P(None, None, 'tp')
Outputs:
- output 1: bfloat16 [128, 1536], P('dp'), parts along dimension 0
- output 2: bfloat16 [128, 128, 8, 64], P('dp', None, 'tp'), parts along dimension 0
- output 3: bfloat16 [128, 128, 8, 64], P('dp', None, 'tp'), parts along dimension 0
- output 4: bfloat16 [128, 128, 8, 64], P('dp', None, 'tp'), parts along dimension 0
- output 5: bfloat16 [128, 128, 8, 64], P('dp', None, 'tp'), parts along dimension 0
There are 4 independent parts. The reference program is written for one: setup_inputs(seed, part) draws one part's arguments, and reference() takes and returns one part's arrays. A program takes and returns all parts, laid end to end along the dimension named above; an argument that names none is the same for every part.
All inputs are finite; a program needn't handle non-finite values.
Results may differ from the reference program's by a relative error of at most 0.02.
Values are sent between devices in bfloat16 or wider.
A program may use at most 768 MiB of HBM per device.

```python
import jax
import jax.numpy as jnp
from jax import lax

BATCH = 32
SEQ = 128
D = 1536
HEADS = 24
KV_HEADS = 8
HEAD = 64
FF = 512
EXPERTS = 40
TOP = 8
LAYERS = 2
EPS = 1e-5
THETA = 1000000.0


def weight_draw(key, shape, fan_in, gain_mult):
    return (jax.random.normal(key, shape, jnp.float32) * (gain_mult * fan_in ** -0.5)).astype(jnp.bfloat16)


def value_walk(key, cache_shape):
    step_key, noise_key = jax.random.split(key)
    walk_steps = jax.random.normal(step_key, cache_shape, jnp.float32) * SEQ ** -0.5
    noise_part = 0.5 * jax.random.normal(noise_key, cache_shape, jnp.float32)
    return (jnp.cumsum(walk_steps, axis=1) + noise_part).astype(jnp.bfloat16)


def setup_inputs(seed: int = 0, part: int = 0) -> dict:
    base_key = jax.random.key(seed)
    shared = jax.random.split(base_key, 11)
    local_keys = jax.random.split(jax.random.fold_in(base_key, part), 9)
    cache_shape = (BATCH, SEQ, KV_HEADS, HEAD)
    hidden = jax.random.normal(local_keys[0], (BATCH, D), jnp.float32).astype(jnp.bfloat16)
    drawn_lens = jax.random.randint(local_keys[1], (BATCH,), 0, SEQ)
    full_row = jax.random.randint(local_keys[2], (), 0, BATCH)
    lengths = jnp.where(jnp.arange(BATCH) == full_row, SEQ - 1, drawn_lens).astype(jnp.int32)
    rank_score = jax.random.randint(local_keys[3], (LAYERS, BATCH, EXPERTS), 0, 2 ** 20) * EXPERTS + jnp.arange(EXPERTS)
    choice = lax.top_k(rank_score, TOP)[1].astype(jnp.int32)
    return {
        'hidden': hidden,
        'lengths': lengths,
        'choice': choice,
        'keys_one': jax.random.normal(local_keys[4], cache_shape, jnp.float32).astype(jnp.bfloat16),
        'vals_one': value_walk(local_keys[5], cache_shape),
        'keys_two': jax.random.normal(local_keys[6], cache_shape, jnp.float32).astype(jnp.bfloat16),
        'vals_two': value_walk(local_keys[7], cache_shape),
        'g_attn': (1.0 + 0.3 * jax.random.normal(shared[0], (LAYERS, D), jnp.float32)).astype(jnp.bfloat16),
        'w_q': weight_draw(shared[1], (LAYERS, D, HEADS * HEAD), D, 1.0),
        'w_k': weight_draw(shared[2], (LAYERS, D, KV_HEADS * HEAD), D, 1.0),
        'w_v': weight_draw(shared[3], (LAYERS, D, KV_HEADS * HEAD), D, 1.0),
        'w_o': weight_draw(shared[4], (LAYERS, HEADS * HEAD, D), HEADS * HEAD, 1.0),
        'g_mlp': (1.0 + 0.3 * jax.random.normal(shared[5], (LAYERS, D), jnp.float32)).astype(jnp.bfloat16),
        'w_router': weight_draw(shared[6], (LAYERS, D, EXPERTS), D, 2.0),
        'w_gate': weight_draw(shared[7], (LAYERS, EXPERTS, D, FF), D, 1.0),
        'w_up': weight_draw(shared[8], (LAYERS, EXPERTS, D, FF), D, 1.0),
        'w_down': weight_draw(shared[9], (LAYERS, EXPERTS, FF, D), FF, 2.0),
    }


def rms_norm(tensor, gain_vec):
    tensor_f = tensor.astype(jnp.float32)
    scale = lax.rsqrt(jnp.mean(tensor_f * tensor_f, axis=-1, keepdims=True) + EPS)
    return (tensor_f * scale * gain_vec.astype(jnp.float32)).astype(jnp.bfloat16)


def apply_rope(tensor, lengths):
    head_dim = tensor.shape[-1]
    half_dim = head_dim // 2
    inv_freq = THETA ** (-2.0 * jnp.arange(half_dim, dtype=jnp.float32) / head_dim)
    angle = lengths.astype(jnp.float32)[:, None] * inv_freq[None, :]
    cos_part = jnp.cos(angle)[:, None, :]
    sin_part = jnp.sin(angle)[:, None, :]
    lower_half = tensor[..., :half_dim]
    upper_half = tensor[..., half_dim:]
    return jnp.concatenate([lower_half * cos_part - upper_half * sin_part, upper_half * cos_part + lower_half * sin_part], axis=-1)


def decode_layer(hidden, lengths, choice, key_cache, val_cache, g_attn, w_q, w_k, w_v, w_o, g_mlp, w_router, w_gate, w_up, w_down):
    batch_rows = hidden.shape[0]
    seq_len = key_cache.shape[1]
    normed = rms_norm(hidden, g_attn)
    query_rot = apply_rope(jnp.dot(normed, w_q, preferred_element_type=jnp.float32).reshape(batch_rows, HEADS, HEAD), lengths).astype(jnp.bfloat16)
    key_new = apply_rope(jnp.dot(normed, w_k, preferred_element_type=jnp.float32).reshape(batch_rows, KV_HEADS, HEAD), lengths).astype(jnp.bfloat16)
    val_new = jnp.dot(normed, w_v, preferred_element_type=jnp.float32).astype(jnp.bfloat16).reshape(batch_rows, KV_HEADS, HEAD)
    positions = jnp.arange(seq_len)
    is_new = (positions[None, :] == lengths[:, None])[:, :, None, None]
    key_cache = jnp.where(is_new, key_new[:, None], key_cache)
    val_cache = jnp.where(is_new, val_new[:, None], val_cache)
    query_grp = query_rot.reshape(batch_rows, KV_HEADS, HEADS // KV_HEADS, HEAD)
    scores = jnp.einsum('bgrd,bsgd->bgrs', query_grp.astype(jnp.float32), key_cache.astype(jnp.float32)) * HEAD ** -0.5
    is_valid = (positions[None, :] <= lengths[:, None])[:, None, None, :]
    attn_prob = jax.nn.softmax(jnp.where(is_valid, scores, -1e30), axis=-1).astype(jnp.bfloat16)
    attn_vec = jnp.einsum('bgrs,bsgd->bgrd', attn_prob.astype(jnp.float32), val_cache.astype(jnp.float32)).astype(jnp.bfloat16).reshape(batch_rows, HEADS * HEAD)
    x_mid = (hidden.astype(jnp.float32) + jnp.dot(attn_vec, w_o, preferred_element_type=jnp.float32)).astype(jnp.bfloat16)
    normed_mid = rms_norm(x_mid, g_mlp)
    logits = jnp.dot(normed_mid, w_router, preferred_element_type=jnp.float32)
    onehot = (choice[:, :, None] == jnp.arange(EXPERTS)[None, None, :]).astype(jnp.float32)
    gate_prob = jax.nn.softmax(jnp.sum(onehot * logits[:, None, :], axis=-1), axis=-1)
    gate_mat = jnp.sum(gate_prob[:, :, None] * onehot, axis=1)
    gate_act = jnp.einsum('bd,edf->bef', normed_mid.astype(jnp.float32), w_gate.astype(jnp.float32))
    up_act = jnp.einsum('bd,edf->bef', normed_mid.astype(jnp.float32), w_up.astype(jnp.float32))
    expert_in = (jax.nn.silu(gate_act) * up_act * gate_mat[:, :, None]).astype(jnp.bfloat16)
    moe_out = jnp.einsum('bef,efd->bd', expert_in.astype(jnp.float32), w_down.astype(jnp.float32))
    return (x_mid.astype(jnp.float32) + moe_out).astype(jnp.bfloat16), key_cache, val_cache


def reference(hidden, lengths, choice, keys_one, vals_one, keys_two, vals_two, g_attn, w_q, w_k, w_v, w_o, g_mlp, w_router, w_gate, w_up, w_down):
    caches = [(keys_one, vals_one), (keys_two, vals_two)]
    results = []
    for layer_idx in range(LAYERS):
        hidden, key_cache, val_cache = decode_layer(hidden, lengths, choice[layer_idx], caches[layer_idx][0], caches[layer_idx][1], g_attn[layer_idx], w_q[layer_idx], w_k[layer_idx], w_v[layer_idx], w_o[layer_idx], g_mlp[layer_idx], w_router[layer_idx], w_gate[layer_idx], w_up[layer_idx], w_down[layer_idx])
        results.append(key_cache)
        results.append(val_cache)
    return (hidden, results[0], results[1], results[2], results[3])
```

```python
import math

import jax
import jax.numpy as jnp
from jax import lax
from jax.experimental import pallas as pl
from jax.experimental.pallas import tpu as pltpu
from jax.sharding import PartitionSpec as P

EPS = 1e-5
THETA = 1000000.0
F32 = jnp.float32
BF16 = jnp.bfloat16
MESH = pl.DeviceIdType.MESH
NT = (((1,), (1,)), ((), ()))
TN = (((0,), (0,)), ((), ()))
CHUNK = 256
VMEM_BYTES = 67043328


def dot_nt(a, b):
    return lax.dot_general(a, b, NT, preferred_element_type=F32)


def iota(shape, dim):
    return lax.broadcasted_iota(jnp.int32, shape, dim)


def rms(h, gain):
    hf = h.astype(F32)
    scale = lax.rsqrt(jnp.mean(hf * hf, axis=-1, keepdims=True) + EPS)
    return (hf * scale * gain.astype(F32)).astype(BF16)


def make_kernel(n, rows, dim, seq, heads, head, experts, ff, top):
    half = rows // 2
    slots = seq // n
    q_heads = heads
    hidden_rows = experts * ff
    chunks = hidden_rows // CHUNK
    cut_cols = dim // (n // 2)
    parts = 3 * experts

    def kernel(hidden, lens, choice, k1, v1, k2, v2, g_attn, wq, wk, wv, wo, g_mlp, wr, wg, wu, wd,
               h_out, o0, o1, o2, o3,
               raw, tmp, send, recv, out_t, wqkv_v, wo_v, wr_v, wg_v, wu_v, wd_v, hs, ga_v, gm_v, ch_v,
               qs, kn, vn, sc, lrow, cosv, sinv, spread, gs_v, act, part, rs,
               raw_sem, small_sem, proj_sem, wg_sem, wu_sem, wd_sem, send_sem, recv_sem,
               rs_send, rs_recv, ag_send, ag_recv, out_sem):
        me = lax.axis_index('tp')
        caches = (k1, v1, k2, v2)
        outs = (o0, o1, o2, o3)

        def peer_of(d):
            return lax.rem(me + d, n)

        def copies_small():
            return [pltpu.make_async_copy(hidden, hs.at[0], small_sem.at[0]),
                    pltpu.make_async_copy(g_attn, ga_v, small_sem.at[1]),
                    pltpu.make_async_copy(g_mlp, gm_v, small_sem.at[2]),
                    pltpu.make_async_copy(choice, ch_v, small_sem.at[3]),
                    pltpu.make_async_copy(wr, wr_v, small_sem.at[4])]

        qw, kw = q_heads * head, head

        def copies_proj(l):
            return [pltpu.make_async_copy(wq.at[l], wqkv_v.at[l, pl.ds(0, qw)], proj_sem.at[l, 0]),
                    pltpu.make_async_copy(wk.at[l], wqkv_v.at[l, pl.ds(qw, kw)], proj_sem.at[l, 1]),
                    pltpu.make_async_copy(wv.at[l], wqkv_v.at[l, pl.ds(qw + kw, kw)], proj_sem.at[l, 2]),
                    pltpu.make_async_copy(wv.at[l], wqkv_v.at[l, pl.ds(qw + 2 * kw, kw)], proj_sem.at[l, 3]),
                    pltpu.make_async_copy(wo.at[l], wo_v.at[l], proj_sem.at[l, 4])]

        def copy_chunk(src, dst, sem, l, c):
            at = pl.ds(pl.multiple_of(c * CHUNK, CHUNK), CHUNK)
            return pltpu.make_async_copy(src.at[l, at], dst.at[l, at], sem.at[l, c])

        barrier = pltpu.get_barrier_semaphore()
        for d in range(1, n):
            pl.semaphore_signal(barrier, inc=1, device_id={'tp': peer_of(d)}, device_id_type=MESH)
        for c in range(2):
            pltpu.make_async_copy(caches[c], raw.at[c], raw_sem.at[c]).start()
        for cp in copies_small():
            cp.start()
        for cp in copies_proj(0):
            cp.start()
        for c in range(2, 4):
            pltpu.make_async_copy(caches[c], raw.at[c], raw_sem.at[c]).start()

        def start_weights(l):
            def go(c, carry):
                copy_chunk(wg, wg_v, wg_sem, l, c).start()
                copy_chunk(wu, wu_v, wu_sem, l, c).start()
                return carry
            lax.fori_loop(0, chunks, go, 0)

            def go_down(c, carry):
                copy_chunk(wd, wd_v, wd_sem, l, c).start()
                return carry
            lax.fori_loop(0, chunks, go_down, 0)

        start_weights(0)
        for cp in copies_proj(1):
            cp.start()
        start_weights(1)

        def pack(c):
            pltpu.make_async_copy(caches[c], raw.at[c], raw_sem.at[c]).wait()

            def step(i, carry):
                for u in range(4):
                    b = i * 4 + u
                    tmp[u, :, 0:head] = raw[c, b].astype(F32).reshape(slots * n, head)
                    tmp[u, :, head:2 * head] = raw[c, b + half].astype(F32).reshape(slots * n, head)
                for u in range(4):
                    b = i * 4 + u
                    for h in range(n):
                        send[c, h, b] = tmp[u, pl.ds(h, slots, stride=n), :].astype(BF16)
                return carry
            lax.fori_loop(0, half // 4, step, 0)

        def exchange(c, d):
            peer = peer_of(d)
            return pltpu.make_async_remote_copy(
                src_ref=send.at[c, peer], dst_ref=recv.at[c, :, me], send_sem=send_sem.at[c, d],
                recv_sem=recv_sem.at[c, me], device_id={'tp': peer}, device_id_type=MESH)

        def landed(c, d):
            peer = peer_of(d)
            return pltpu.make_async_remote_copy(
                src_ref=send.at[c, peer], dst_ref=recv.at[c, :, peer], send_sem=send_sem.at[c, d],
                recv_sem=recv_sem.at[c, peer], device_id={'tp': peer}, device_id_type=MESH)

        def send_cache(c):
            for d in range(1, n):
                exchange(c, d).start()

            def own(b, carry):
                recv[c, b, me] = send[c, me, b]
                return carry
            lax.fori_loop(0, half, own, 0)

        def wait_cache(c):
            for d in range(1, n):
                landed(c, d).wait_recv()

        pack(0)
        pl.semaphore_wait(barrier, n - 1)
        send_cache(0)
        pack(1)
        send_cache(1)

        for cp in copies_small():
            cp.wait()

        lane_c = iota((rows, 2 * head), 1)
        row_c = iota((rows, 2 * head), 0)
        len_c = jnp.zeros((rows, 2 * head), jnp.int32)
        for b in range(rows):
            len_c = jnp.where(row_c == b, lens[b], len_c)
        freq = jnp.exp((lane_c & (head // 2 - 1)).astype(F32) * (-2.0 * math.log(THETA) / head))
        angle = len_c.astype(F32) * freq
        cosv[...] = jnp.cos(angle)
        sine = jnp.sin(angle)
        lower = (lane_c & (head - 1)) < head // 2
        sinv[...] = jnp.where(lower, -sine, sine)
        row8 = iota((8, seq), 0)
        for b in range(half):
            lrow[pl.ds(8 * b, 8), :] = jnp.where(row8 < 4, lens[b], lens[b + half])
        part_row = iota((128, CHUNK), 0)
        part_e = jnp.where(part_row >= 2 * experts, part_row - 2 * experts,
                           jnp.where(part_row >= experts, part_row - experts, part_row))
        part_e = jnp.where(part_row >= parts, -1, part_e)
        col_e = iota((128, CHUNK), 1) // ff
        for c in range(chunks):
            spread[c] = jnp.where(part_e == col_e + c * (CHUNK // ff), 1.0, 0.0).astype(BF16)
        qs[...] = jnp.zeros_like(qs)

        lane16 = iota((half, 2 * head), 1)
        left16 = lane16 < head

        def swap(x):
            return pltpu.roll(x, head, 1)

        def rope(x):
            partner = jnp.where(lower, pltpu.roll(x, 2 * head - head // 2, 1), pltpu.roll(x, head // 2, 1))
            return (x * cosv[...] + partner * sinv[...]).astype(BF16).astype(F32)

        def project(l):
            for cp in copies_proj(l):
                cp.wait()
            a = rms(hs[2 * l], ga_v[l:l + 1, :])
            qkv = dot_nt(a, wqkv_v[l])
            t0 = rope(qkv[:, 0:2 * head])
            t1 = rope(qkv[:, 2 * head:4 * head])
            t2 = qkv[:, 4 * head:6 * head].astype(BF16).astype(F32)
            s0, s1 = swap(t0), swap(t1)
            zero = jnp.zeros((half, 2 * head), F32)
            qs[pl.ds(0, half, stride=8), :] = jnp.where(left16, t0[0:half], zero)
            qs[pl.ds(1, half, stride=8), :] = jnp.where(left16, s0[0:half], zero)
            qs[pl.ds(2, half, stride=8), :] = jnp.where(left16, t1[0:half], zero)
            qs[pl.ds(4, half, stride=8), :] = jnp.where(left16, zero, s0[half:rows])
            qs[pl.ds(5, half, stride=8), :] = jnp.where(left16, zero, t0[half:rows])
            qs[pl.ds(6, half, stride=8), :] = jnp.where(left16, zero, s1[half:rows])
            kn[...] = jnp.where(left16, s1[0:half], t1[half:rows])
            vn[...] = jnp.where(left16, t2[0:half], t2[half:rows])

        pos = iota((seq, 2 * head), 0)
        left_s = iota((seq, 2 * head), 1) < head

        def insert(c, b, new):
            at = jnp.where(left_s, lens[b], lens[b + half])
            x = recv[c, b].astype(F32).reshape(seq, 2 * head)
            x = jnp.where(pos == at, new[pl.ds(b, 1), :], x).astype(BF16)
            recv[c, b] = x.reshape(n, slots, 2 * head)
            return x

        def attend(l):
            kc, vc = 2 * l, 2 * l + 1
            wait_cache(kc)

            def k_step(i, carry):
                for u in range(4):
                    b = i * 4 + u
                    x = insert(kc, b, kn)
                    at = pl.ds(pl.multiple_of(b * 8, 8), 8)
                    sc[at, :] = dot_nt(qs[at, :].astype(BF16), x)
                return carry
            lax.fori_loop(0, half // 4, k_step, 0)
            s = sc[...] * head ** -0.5
            valid = iota((8 * half, seq), 1) <= lrow[...]
            s = jnp.where(valid, s, -1e30)
            e = jnp.exp(s - jnp.max(s, axis=-1, keepdims=True))
            sc[...] = e / jnp.sum(e, axis=-1, keepdims=True)
            wait_cache(vc)

            def v_step(i, carry):
                for u in range(4):
                    b = i * 4 + u
                    x = insert(vc, b, vn)
                    at = pl.ds(pl.multiple_of(b * 8, 8), 8)
                    sc[at, :] = jnp.dot(sc[at, :].astype(BF16), x, preferred_element_type=F32)
                return carry
            lax.fori_loop(0, half // 4, v_step, 0)
            up = [sc[pl.ds(j, half, stride=8), :] for j in range(3)]
            dn = [sc[pl.ds(4 + j, half, stride=8), :] for j in range(3)]
            t0 = jnp.concatenate([jnp.where(left16, up[0], swap(up[1])), jnp.where(left16, swap(dn[0]), dn[1])], axis=0)
            t1 = jnp.concatenate([up[2], swap(dn[2])], axis=0)
            t0 = t0.astype(BF16)
            t1 = t1[:, 0:head].astype(BF16)
            return (jnp.dot(t0, wo_v[l, 0:2 * head, :], preferred_element_type=F32)
                    + jnp.dot(t1, wo_v[l, 2 * head:3 * head, :], preferred_element_type=F32))

        def piece(p):
            return (pl.ds(pl.multiple_of((p // (n // 2)) * half, half), half),
                    pl.ds(pl.multiple_of((p % (n // 2)) * cut_cols, 128), cut_cols))

        def rs_copy(ar, d, src_slot):
            peer = peer_of(d)
            r, c = piece(peer)
            return pltpu.make_async_remote_copy(
                src_ref=part.at[ar, r, c], dst_ref=rs.at[ar, src_slot], send_sem=rs_send.at[ar, d],
                recv_sem=rs_recv.at[ar, src_slot], device_id={'tp': peer}, device_id_type=MESH)

        def ag_copy(ar, d, owner):
            peer = peer_of(d)
            r, c = piece(owner)
            return pltpu.make_async_remote_copy(
                src_ref=hs.at[ar + 1, r, c], dst_ref=hs.at[ar + 1, r, c], send_sem=ag_send.at[ar, d],
                recv_sem=ag_recv.at[ar, owner], device_id={'tp': peer}, device_id_type=MESH)

        def reduce_start(ar):
            for d in range(1, n):
                rs_copy(ar, d, me).start()

        def reduce_finish(ar):
            r, c = piece(me)
            acc = part[ar, r, c].astype(F32)
            for d in range(1, n):
                rs_copy(ar, d, peer_of(d)).wait_recv()
                acc = acc + rs[ar, peer_of(d)].astype(F32)
            hs[ar + 1, r, c] = (hs[ar, r, c].astype(F32) + acc).astype(BF16)
            for d in range(1, n):
                ag_copy(ar, d, me).start()

        def gather_finish(ar):
            for d in range(1, n):
                ag_copy(ar, d, peer_of(d)).wait_recv()

        def transpose_out(c):
            def step(i, carry):
                for u in range(2):
                    b = i * 2 + u
                    x = recv[c, b].astype(F32).reshape(seq, 2 * head).T.astype(BF16)
                    out_t[c, b] = x[0:head]
                    out_t[c, b + half] = x[head:2 * head]
                return carry
            lax.fori_loop(0, half // 2, step, 0)
            pltpu.make_async_copy(out_t.at[c], outs[c], out_sem.at[c]).start()

        def experts_of(l):
            m = rms(hs[2 * l + 1], gm_v[l:l + 1, :])
            logits = dot_nt(wr_v[l], m)
            row_e = iota((experts, rows), 0)
            picked = row_e == ch_v[l, 0:1, :]
            for t in range(1, top):
                picked = jnp.logical_or(picked, row_e == ch_v[l, t:t + 1, :])
            lg = jnp.where(picked, logits, -1e30)
            e = jnp.where(picked, jnp.exp(lg - jnp.max(lg, axis=0, keepdims=True)), 0.0)
            gate = e / jnp.sum(e, axis=0, keepdims=True)
            hi = gate.astype(BF16).astype(F32)
            mid = (gate - hi).astype(BF16).astype(F32)
            lo = (gate - hi - mid).astype(BF16).astype(F32)
            pad = jnp.zeros((128 - parts, rows), F32)
            gs_v[...] = jnp.concatenate([hi, mid, lo, pad], axis=0)
            gst = gs_v[...].astype(BF16)

            def up_step(c, carry):
                at = pl.ds(pl.multiple_of(c * CHUNK, CHUNK), CHUNK)
                copy_chunk(wg, wg_v, wg_sem, l, c).wait()
                copy_chunk(wu, wu_v, wu_sem, l, c).wait()
                g = dot_nt(m, wg_v[l, at, :])
                u = dot_nt(m, wu_v[l, at, :])
                w = lax.dot_general(gst, spread[c], TN, preferred_element_type=F32)
                act[c] = (g * jax.nn.sigmoid(g) * u * w).astype(BF16)
                return carry
            lax.fori_loop(0, chunks, up_step, 0)

            def wait_down(c, carry):
                copy_chunk(wd, wd_v, wd_sem, l, c).wait()
                return carry
            lax.fori_loop(0, chunks, wait_down, 0)
            u_all = jnp.concatenate([act[c] for c in range(chunks)], axis=1)

            def down_step(j, carry):
                at = pl.ds(pl.multiple_of(j * 256, 256), 256)
                y = jnp.dot(u_all, wd_v[l, :, at], preferred_element_type=F32)
                part[2 * l + 1, :, at] = y.astype(BF16)
                return carry
            lax.fori_loop(0, dim // 256, down_step, 0)

        for l in range(2):
            project(l)
            if l == 0:
                pack(2)
                send_cache(2)
            part[2 * l] = attend(l).astype(BF16)
            reduce_start(2 * l)
            if l == 0:
                pack(3)
                send_cache(3)
            reduce_finish(2 * l)
            transpose_out(2 * l)
            gather_finish(2 * l)
            experts_of(l)
            reduce_start(2 * l + 1)
            transpose_out(2 * l + 1)
            reduce_finish(2 * l + 1)
            gather_finish(2 * l + 1)

        final = pltpu.make_async_copy(hs.at[4], h_out, small_sem.at[0])
        final.start()
        for c in range(4):
            for d in range(1, n):
                exchange(c, d).wait_send()
        for ar in range(4):
            for d in range(1, n):
                rs_copy(ar, d, me).wait_send()
                ag_copy(ar, d, me).wait_send()
        for c in range(4):
            pltpu.make_async_copy(out_t.at[c], outs[c], out_sem.at[c]).wait()
        final.wait()

    return kernel


def solution(mesh):
    n = mesh.shape['tp']
    seq_spec = P('dp', 'tp', None, None)
    head_spec = P('dp', None, 'tp', None)
    col_spec = P(None, None, 'tp')
    ff_spec = P(None, None, None, 'tp')

    def local_step(hidden, lengths, choice, keys_one, vals_one, keys_two, vals_two, g_attn, w_q, w_k, w_v, w_o, g_mlp, w_router, w_gate, w_up, w_down):
        rows, dim = hidden.shape
        slots, head = keys_one.shape[1], keys_one.shape[3]
        seq = slots * n
        heads = w_q.shape[2] // head
        experts, ff = w_gate.shape[1], w_gate.shape[3]
        top = choice.shape[2]
        half = rows // 2
        hidden_rows = experts * ff
        chunks = hidden_rows // CHUNK
        cache_out = jax.ShapeDtypeStruct((rows, head, seq), BF16)
        dma = pltpu.SemaphoreType.DMA
        any_spec = pl.BlockSpec(memory_space=pl.ANY)
        smem_spec = pl.BlockSpec(memory_space=pltpu.SMEM)
        flip = lambda w: jnp.swapaxes(w, -1, -2)
        flat = lambda w: w.reshape(w.shape[0], hidden_rows, dim)
        outs = pl.pallas_call(
            make_kernel(n, rows, dim, seq, heads, head, experts, ff, top),
            out_shape=[jax.ShapeDtypeStruct((rows, dim), BF16)] + [cache_out] * 4,
            in_specs=[any_spec, smem_spec] + [any_spec] * 15,
            out_specs=[any_spec] * 5,
            scratch_shapes=[
                pltpu.VMEM((4, rows, slots, n, head), BF16),
                pltpu.VMEM((4, slots * n, 2 * head), F32),
                pltpu.VMEM((4, n, half, slots, 2 * head), BF16),
                pltpu.VMEM((4, half, n, slots, 2 * head), BF16),
                pltpu.VMEM((4, rows, head, seq), BF16),
                pltpu.VMEM((2, (heads + 3) * head, dim), BF16),
                pltpu.VMEM((2, heads * head, dim), BF16),
                pltpu.VMEM((2, experts, dim), BF16),
                pltpu.VMEM((2, hidden_rows, dim), BF16),
                pltpu.VMEM((2, hidden_rows, dim), BF16),
                pltpu.VMEM((2, hidden_rows, dim), BF16),
                pltpu.VMEM((5, rows, dim), BF16),
                pltpu.VMEM((2, dim), BF16),
                pltpu.VMEM((2, dim), BF16),
                pltpu.VMEM((2, top, rows), jnp.int32),
                pltpu.VMEM((8 * half, 2 * head), F32),
                pltpu.VMEM((half, 2 * head), F32),
                pltpu.VMEM((half, 2 * head), F32),
                pltpu.VMEM((8 * half, seq), F32),
                pltpu.VMEM((8 * half, seq), jnp.int32),
                pltpu.VMEM((rows, 2 * head), F32),
                pltpu.VMEM((rows, 2 * head), F32),
                pltpu.VMEM((chunks, 128, CHUNK), BF16),
                pltpu.VMEM((128, rows), F32),
                pltpu.VMEM((chunks, rows, CHUNK), BF16),
                pltpu.VMEM((4, rows, dim), BF16),
                pltpu.VMEM((4, n, half, dim // (n // 2)), BF16),
                dma((4,)), dma((5,)), dma((2, 5)), dma((2, chunks)), dma((2, chunks)), dma((2, chunks)),
                dma((4, n)), dma((4, n)), dma((4, n)), dma((4, n)), dma((4, n)), dma((4, n)), dma((4,)),
            ],
            compiler_params=pltpu.CompilerParams(
                collective_id=0, has_side_effects=True, vmem_limit_bytes=VMEM_BYTES),
            name='decode_two_layers',
        )(hidden, lengths, flip(choice), keys_one, vals_one, keys_two, vals_two, g_attn,
          flip(w_q), flip(w_k), flip(w_v), w_o, g_mlp, flip(w_router),
          flat(flip(w_gate)), flat(flip(w_up)), flat(w_down))
        back = lambda o: flip(o)[:, :, None, :]
        return (outs[0], back(outs[1]), back(outs[2]), back(outs[3]), back(outs[4]))

    return jax.shard_map(local_step, mesh=mesh, in_specs=(P('dp', None), P('dp'), P(None, 'dp', None), seq_spec, seq_spec, seq_spec, seq_spec, P(), col_spec, col_spec, col_spec, P(None, 'tp', None), P(), P(), ff_spec, ff_spec, P(None, None, 'tp', None)), out_specs=(P('dp', None), head_spec, head_spec, head_spec, head_spec), check_vma=False)
```

```python
import math

import jax
import jax.numpy as jnp
from jax import lax
from jax.experimental import pallas as pl
from jax.experimental.pallas import tpu as pltpu
from jax.sharding import PartitionSpec as P

EPS = 1e-5
THETA = 1000000.0
F32 = jnp.float32
BF16 = jnp.bfloat16
MESH = pl.DeviceIdType.MESH
NT = (((1,), (1,)), ((), ()))
TN = (((0,), (0,)), ((), ()))
CHUNK = 256
UP_UNROLL = 10
DOWN_UNROLL = 6
DOWN = 256
VMEM_BYTES = 67043328


def dot_nt(a, b):
    return lax.dot_general(a, b, NT, preferred_element_type=F32)


def iota(shape, dim):
    return lax.broadcasted_iota(jnp.int32, shape, dim)


def rms(h, gain):
    hf = h.astype(F32)
    scale = lax.rsqrt(jnp.mean(hf * hf, axis=-1, keepdims=True) + EPS)
    return (hf * scale * gain.astype(F32)).astype(BF16)


def make_kernel(n, rows, dim, seq, heads, head, experts, ff, top):
    half = rows // 2
    slots = seq // n
    q_heads = heads
    hidden_rows = experts * ff
    chunks = hidden_rows // CHUNK
    cut_cols = dim // (n // 2)
    parts = 3 * experts

    def kernel(hidden, lens, choice, k1, v1, k2, v2, g_attn, wq, wk, wv, wo, g_mlp, wr, wg, wu, wd,
               h_out, o0, o1, o2, o3,
               raw, tmp, send, recv, out_t, wqkv_v, wo_v, wr_v, wg_v, wu_v, wd_v, hs, ga_v, gm_v, ch_v,
               qs, kn, vn, sc, lrow, cosv, sinv, spread, gs_v, act, part, rs,
               raw_sem, small_sem, proj_sem, wg_sem, wu_sem, wd_sem, send_sem, recv_sem,
               rs_send, rs_recv, ag_send, ag_recv, out_sem):
        me = lax.axis_index('tp')
        caches = (k1, v1, k2, v2)
        outs = (o0, o1, o2, o3)

        def peer_of(d):
            return lax.rem(me + d, n)

        def copies_small():
            return [pltpu.make_async_copy(hidden, hs.at[0], small_sem.at[0]),
                    pltpu.make_async_copy(g_attn, ga_v, small_sem.at[1]),
                    pltpu.make_async_copy(g_mlp, gm_v, small_sem.at[2]),
                    pltpu.make_async_copy(choice, ch_v, small_sem.at[3]),
                    pltpu.make_async_copy(wr, wr_v, small_sem.at[4])]

        qw, kw = q_heads * head, head

        def copies_proj(l):
            return [pltpu.make_async_copy(wq.at[l], wqkv_v.at[l, pl.ds(0, qw)], proj_sem.at[l, 0]),
                    pltpu.make_async_copy(wk.at[l], wqkv_v.at[l, pl.ds(qw, kw)], proj_sem.at[l, 1]),
                    pltpu.make_async_copy(wv.at[l], wqkv_v.at[l, pl.ds(qw + kw, kw)], proj_sem.at[l, 2]),
                    pltpu.make_async_copy(wv.at[l], wqkv_v.at[l, pl.ds(qw + 2 * kw, kw)], proj_sem.at[l, 3]),
                    pltpu.make_async_copy(wo.at[l], wo_v.at[l], proj_sem.at[l, 4])]

        def copy_chunk(src, dst, sem, l, c):
            at = pl.ds(pl.multiple_of(c * CHUNK, CHUNK), CHUNK)
            return pltpu.make_async_copy(src.at[l, at], dst.at[l, at], sem.at[l, c])

        barrier = pltpu.get_barrier_semaphore()
        for d in range(1, n):
            pl.semaphore_signal(barrier, inc=1, device_id={'tp': peer_of(d)}, device_id_type=MESH)
        for c in range(2):
            pltpu.make_async_copy(caches[c], raw.at[c], raw_sem.at[c]).start()
        for cp in copies_small():
            cp.start()
        for cp in copies_proj(0):
            cp.start()
        for c in range(2, 4):
            pltpu.make_async_copy(caches[c], raw.at[c], raw_sem.at[c]).start()

        def start_weights(l):
            def go(c, carry):
                copy_chunk(wg, wg_v, wg_sem, l, c).start()
                copy_chunk(wu, wu_v, wu_sem, l, c).start()
                return carry
            lax.fori_loop(0, chunks, go, 0)

            def go_down(c, carry):
                copy_chunk(wd, wd_v, wd_sem, l, c).start()
                return carry
            lax.fori_loop(0, chunks, go_down, 0)

        start_weights(0)
        for cp in copies_proj(1):
            cp.start()
        start_weights(1)

        def pack(c):
            pltpu.make_async_copy(caches[c], raw.at[c], raw_sem.at[c]).wait()

            def step(i, carry):
                for u in range(4):
                    b = i * 4 + u
                    tmp[u, :, 0:head] = raw[c, b].astype(F32).reshape(slots * n, head)
                    tmp[u, :, head:2 * head] = raw[c, b + half].astype(F32).reshape(slots * n, head)
                for u in range(4):
                    b = i * 4 + u
                    for h in range(n):
                        send[c, h, b] = tmp[u, pl.ds(h, slots, stride=n), :].astype(BF16)
                return carry
            lax.fori_loop(0, half // 4, step, 0)

        quarter = half // 2

        def exchange(c, d, k, owner):
            peer = peer_of(d)
            at = pl.ds(k * quarter, quarter)
            return pltpu.make_async_remote_copy(
                src_ref=send.at[c, peer, at], dst_ref=recv.at[c, at, owner], send_sem=send_sem.at[c, k, d],
                recv_sem=recv_sem.at[c, k, owner], device_id={'tp': peer}, device_id_type=MESH)

        def send_half(c, k):
            for d in range(1, n):
                exchange(c, d, k, me).start()

        def keep_own(c):
            def own(b, carry):
                recv[c, b, me] = send[c, me, b]
                return carry
            lax.fori_loop(0, half, own, 0)

        def send_cache(c):
            send_half(c, 0)
            send_half(c, 1)
            keep_own(c)

        def wait_cache(c):
            for k in range(2):
                for d in range(1, n):
                    exchange(c, d, k, peer_of(d)).wait_recv()

        with jax.named_scope('pack_0'):
            pack(0)
        with jax.named_scope('enter'):
            pl.semaphore_wait(barrier, n - 1)
        with jax.named_scope('send_0'):
            send_cache(0)
        with jax.named_scope('pack_1'):
            pack(1)
        with jax.named_scope('send_1'):
            send_cache(1)

        for cp in copies_small():
            cp.wait()

        tables = jax.named_scope('tables')
        tables.__enter__()
        lane_c = iota((rows, 2 * head), 1)
        row_c = iota((rows, 2 * head), 0)
        len_c = jnp.zeros((rows, 2 * head), jnp.int32)
        for b in range(rows):
            len_c = jnp.where(row_c == b, lens[b], len_c)
        freq = jnp.exp((lane_c & (head // 2 - 1)).astype(F32) * (-2.0 * math.log(THETA) / head))
        angle = len_c.astype(F32) * freq
        cosv[...] = jnp.cos(angle)
        sine = jnp.sin(angle)
        lower = (lane_c & (head - 1)) < head // 2
        sinv[...] = jnp.where(lower, -sine, sine)
        row8 = iota((8, seq), 0)
        for b in range(half):
            lrow[pl.ds(8 * b, 8), :] = jnp.where(row8 < 4, lens[b], lens[b + half])
        part_row = iota((128, CHUNK), 0)
        part_e = jnp.where(part_row >= 2 * experts, part_row - 2 * experts,
                           jnp.where(part_row >= experts, part_row - experts, part_row))
        part_e = jnp.where(part_row >= parts, -1, part_e)
        col_e = iota((128, CHUNK), 1) // ff
        for c in range(chunks):
            spread[c] = jnp.where(part_e == col_e + c * (CHUNK // ff), 1.0, 0.0).astype(BF16)
        qs[...] = jnp.zeros_like(qs)
        tables.__exit__(None, None, None)

        lane16 = iota((half, 2 * head), 1)
        left16 = lane16 < head

        def swap(x):
            return pltpu.roll(x, head, 1)

        def rope(x):
            partner = jnp.where(lower, pltpu.roll(x, 2 * head - head // 2, 1), pltpu.roll(x, head // 2, 1))
            return (x * cosv[...] + partner * sinv[...]).astype(BF16).astype(F32)

        def project(l):
            for cp in copies_proj(l):
                cp.wait()
            a = rms(hs[2 * l], ga_v[l:l + 1, :])
            qkv = dot_nt(a, wqkv_v[l])
            t0 = rope(qkv[:, 0:2 * head])
            t1 = rope(qkv[:, 2 * head:4 * head])
            t2 = qkv[:, 4 * head:6 * head].astype(BF16).astype(F32)
            s0, s1 = swap(t0), swap(t1)
            zero = jnp.zeros((half, 2 * head), F32)
            qs[pl.ds(0, half, stride=8), :] = jnp.where(left16, t0[0:half], zero)
            qs[pl.ds(1, half, stride=8), :] = jnp.where(left16, s0[0:half], zero)
            qs[pl.ds(2, half, stride=8), :] = jnp.where(left16, t1[0:half], zero)
            qs[pl.ds(4, half, stride=8), :] = jnp.where(left16, zero, s0[half:rows])
            qs[pl.ds(5, half, stride=8), :] = jnp.where(left16, zero, t0[half:rows])
            qs[pl.ds(6, half, stride=8), :] = jnp.where(left16, zero, s1[half:rows])
            kn[...] = jnp.where(left16, s1[0:half], t1[half:rows])
            vn[...] = jnp.where(left16, t2[0:half], t2[half:rows])

        pos = iota((seq, 2 * head), 0)
        left_s = iota((seq, 2 * head), 1) < head

        def insert(c, b, new):
            at = jnp.where(left_s, lens[b], lens[b + half])
            x = recv[c, b].astype(F32).reshape(seq, 2 * head)
            x = jnp.where(pos == at, new[pl.ds(b, 1), :], x).astype(BF16)
            recv[c, b] = x.reshape(n, slots, 2 * head)
            return x

        def attend(l):
            kc, vc = 2 * l, 2 * l + 1
            with jax.named_scope(f'wait_k{l}'):
                wait_cache(kc)

            def k_step(i, carry):
                for u in range(4):
                    b = i * 4 + u
                    x = insert(kc, b, kn)
                    at = pl.ds(pl.multiple_of(b * 8, 8), 8)
                    sc[at, :] = dot_nt(qs[at, :].astype(BF16), x)
                return carry
            lax.fori_loop(0, half // 4, k_step, 0)
            s = sc[...] * head ** -0.5
            valid = iota((8 * half, seq), 1) <= lrow[...]
            s = jnp.where(valid, s, -1e30)
            e = jnp.exp(s - jnp.max(s, axis=-1, keepdims=True))
            sc[...] = e / jnp.sum(e, axis=-1, keepdims=True)
            with jax.named_scope(f'wait_v{l}'):
                wait_cache(vc)

            def v_step(i, carry):
                for u in range(4):
                    b = i * 4 + u
                    x = insert(vc, b, vn)
                    at = pl.ds(pl.multiple_of(b * 8, 8), 8)
                    sc[at, :] = jnp.dot(sc[at, :].astype(BF16), x, preferred_element_type=F32)
                return carry
            lax.fori_loop(0, half // 4, v_step, 0)
            up = [sc[pl.ds(j, half, stride=8), :] for j in range(3)]
            dn = [sc[pl.ds(4 + j, half, stride=8), :] for j in range(3)]
            t0 = jnp.concatenate([jnp.where(left16, up[0], swap(up[1])), jnp.where(left16, swap(dn[0]), dn[1])], axis=0)
            t1 = jnp.concatenate([up[2], swap(dn[2])], axis=0)
            t0 = t0.astype(BF16)
            t1 = t1[:, 0:head].astype(BF16)
            return (jnp.dot(t0, wo_v[l, 0:2 * head, :], preferred_element_type=F32)
                    + jnp.dot(t1, wo_v[l, 2 * head:3 * head, :], preferred_element_type=F32))

        def piece(p):
            return (pl.ds(pl.multiple_of((p // (n // 2)) * half, half), half),
                    pl.ds(pl.multiple_of((p % (n // 2)) * cut_cols, 128), cut_cols))

        def rs_copy(ar, d, src_slot):
            peer = peer_of(d)
            r, c = piece(peer)
            return pltpu.make_async_remote_copy(
                src_ref=part.at[ar, r, c], dst_ref=rs.at[ar, src_slot], send_sem=rs_send.at[ar, d],
                recv_sem=rs_recv.at[ar, src_slot], device_id={'tp': peer}, device_id_type=MESH)

        def ag_copy(ar, d, owner):
            peer = peer_of(d)
            r, c = piece(owner)
            return pltpu.make_async_remote_copy(
                src_ref=hs.at[ar + 1, r, c], dst_ref=hs.at[ar + 1, r, c], send_sem=ag_send.at[ar, d],
                recv_sem=ag_recv.at[ar, owner], device_id={'tp': peer}, device_id_type=MESH)

        def reduce_start(ar):
            for d in range(1, n):
                rs_copy(ar, d, me).start()

        def reduce_finish(ar):
            r, c = piece(me)
            acc = part[ar, r, c].astype(F32)
            for d in range(1, n):
                rs_copy(ar, d, peer_of(d)).wait_recv()
                acc = acc + rs[ar, peer_of(d)].astype(F32)
            hs[ar + 1, r, c] = (hs[ar, r, c].astype(F32) + acc).astype(BF16)
            for d in range(1, n):
                ag_copy(ar, d, me).start()

        def gather_finish(ar):
            for d in range(1, n):
                ag_copy(ar, d, peer_of(d)).wait_recv()

        def transpose_out(c):
            def step(i, carry):
                for u in range(2):
                    b = i * 2 + u
                    x = recv[c, b].astype(F32).reshape(seq, 2 * head).T.astype(BF16)
                    out_t[c, b] = x[0:head]
                    out_t[c, b + half] = x[head:2 * head]
                return carry
            lax.fori_loop(0, half // 2, step, 0)
            pltpu.make_async_copy(out_t.at[c], outs[c], out_sem.at[c]).start()

        def experts_of(l):
            gate_scope = jax.named_scope(f'gate_{l}')
            gate_scope.__enter__()
            m = rms(hs[2 * l + 1], gm_v[l:l + 1, :])
            logits = dot_nt(wr_v[l], m)
            row_e = iota((experts, rows), 0)
            picked = row_e == ch_v[l, 0:1, :]
            for t in range(1, top):
                picked = jnp.logical_or(picked, row_e == ch_v[l, t:t + 1, :])
            lg = jnp.where(picked, logits, -1e30)
            e = jnp.where(picked, jnp.exp(lg - jnp.max(lg, axis=0, keepdims=True)), 0.0)
            gate = e / jnp.sum(e, axis=0, keepdims=True)
            hi = gate.astype(BF16).astype(F32)
            mid = (gate - hi).astype(BF16).astype(F32)
            lo = (gate - hi - mid).astype(BF16).astype(F32)
            pad = jnp.zeros((128 - parts, rows), F32)
            gs_v[...] = jnp.concatenate([hi, mid, lo, pad], axis=0)
            gst = gs_v[...].astype(BF16)
            gate_scope.__exit__(None, None, None)

            def up_step(c, carry):
                at = pl.ds(pl.multiple_of(c * CHUNK, CHUNK), CHUNK)
                copy_chunk(wg, wg_v, wg_sem, l, c).wait()
                copy_chunk(wu, wu_v, wu_sem, l, c).wait()
                g = dot_nt(m, wg_v[l, at, :])
                u = dot_nt(m, wu_v[l, at, :])
                w = lax.dot_general(gst, spread[c], TN, preferred_element_type=F32)
                act[c] = (g * jax.nn.sigmoid(g) * u * w).astype(BF16)
                return carry
            with jax.named_scope(f'up_{l}'):
                lax.fori_loop(0, chunks, up_step, 0, unroll=UP_UNROLL)

            def wait_down(c, carry):
                copy_chunk(wd, wd_v, wd_sem, l, c).wait()
                return carry
            lax.fori_loop(0, chunks, wait_down, 0)
            u_all = jnp.concatenate([act[c] for c in range(chunks)], axis=1)

            def down_step(j, carry):
                at = pl.ds(pl.multiple_of(j * DOWN, DOWN), DOWN)
                y = jnp.dot(u_all, wd_v[l, :, at], preferred_element_type=F32)
                part[2 * l + 1, :, at] = y.astype(BF16)
                return carry
            with jax.named_scope(f'down_{l}'):
                lax.fori_loop(0, dim // DOWN, down_step, 0, unroll=DOWN_UNROLL)

        for l in range(2):
            with jax.named_scope(f'project_{l}'):
                project(l)
            with jax.named_scope(f'attend_{l}'):
                part[2 * l] = attend(l).astype(BF16)
            with jax.named_scope(f'rs_a{l}'):
                reduce_start(2 * l)
            if l == 0:
                with jax.named_scope('pack_2'):
                    pack(2)
                    send_half(2, 0)
            with jax.named_scope(f'rs_a{l}_fin'):
                reduce_finish(2 * l)
            if l == 0:
                with jax.named_scope('pack_3'):
                    send_half(2, 1)
                    keep_own(2)
                    pack(3)
            with jax.named_scope(f'tr_a{l}'):
                transpose_out(2 * l)
            with jax.named_scope(f'ag_a{l}'):
                gather_finish(2 * l)
            if l == 0:
                send_half(3, 0)
                send_half(3, 1)
                keep_own(3)
            experts_of(l)
            with jax.named_scope(f'rs_m{l}'):
                reduce_start(2 * l + 1)
            with jax.named_scope(f'tr_m{l}'):
                transpose_out(2 * l + 1)
            with jax.named_scope(f'rs_m{l}_fin'):
                reduce_finish(2 * l + 1)
            with jax.named_scope(f'ag_m{l}'):
                gather_finish(2 * l + 1)

        final = pltpu.make_async_copy(hs.at[4], h_out, small_sem.at[0])
        final.start()
        tail = jax.named_scope('tail')
        tail.__enter__()
        for c in range(4):
            for k in range(2):
                for d in range(1, n):
                    exchange(c, d, k, me).wait_send()
        for ar in range(4):
            for d in range(1, n):
                rs_copy(ar, d, me).wait_send()
                ag_copy(ar, d, me).wait_send()
        for c in range(4):
            pltpu.make_async_copy(out_t.at[c], outs[c], out_sem.at[c]).wait()
        final.wait()
        tail.__exit__(None, None, None)

    return kernel


def pass_on(*refs):
    src, dst, mid, in_sem, out_sem = refs[0:5], refs[5:10], refs[10:15], refs[15], refs[16]

    def part(ref, k):
        size = ref.shape[0] // 2
        return ref.at[pl.ds(k * size, size)]

    moves = [(i, k) for i in range(5) for k in range(2)]
    into = [pltpu.make_async_copy(part(src[i], k), part(mid[i], k), in_sem.at[i, k]) for i, k in moves]
    away = [pltpu.make_async_copy(part(mid[i], k), part(dst[i], k), out_sem.at[i, k]) for i, k in moves]
    for cp in into:
        cp.start()
    for a, b in zip(into, away):
        a.wait()
        b.start()
    for cp in away:
        cp.wait()


def solution(mesh):
    n = mesh.shape['tp']
    seq_spec = P('dp', 'tp', None, None)
    head_spec = P('dp', None, 'tp', None)
    col_spec = P(None, None, 'tp')
    ff_spec = P(None, None, None, 'tp')

    def local_step(hidden, lengths, choice, keys_one, vals_one, keys_two, vals_two, g_attn, w_q, w_k, w_v, w_o, g_mlp, w_router, w_gate, w_up, w_down):
        rows, dim = hidden.shape
        slots, head = keys_one.shape[1], keys_one.shape[3]
        seq = slots * n
        heads = w_q.shape[2] // head
        experts, ff = w_gate.shape[1], w_gate.shape[3]
        top = choice.shape[2]
        half = rows // 2
        hidden_rows = experts * ff
        chunks = hidden_rows // CHUNK
        cache_out = jax.ShapeDtypeStruct((rows, head, seq), BF16)
        dma = pltpu.SemaphoreType.DMA
        any_spec = pl.BlockSpec(memory_space=pl.ANY)
        smem_spec = pl.BlockSpec(memory_space=pltpu.SMEM)
        flip = lambda w: jnp.swapaxes(w, -1, -2)
        flat = lambda w: w.reshape(w.shape[0], hidden_rows, dim)
        outs = pl.pallas_call(
            make_kernel(n, rows, dim, seq, heads, head, experts, ff, top),
            out_shape=[jax.ShapeDtypeStruct((rows, dim), BF16)] + [cache_out] * 4,
            in_specs=[any_spec, smem_spec] + [any_spec] * 15,
            out_specs=[any_spec] * 5,
            scratch_shapes=[
                pltpu.VMEM((4, rows, slots, n, head), BF16),
                pltpu.VMEM((4, slots * n, 2 * head), F32),
                pltpu.VMEM((4, n, half, slots, 2 * head), BF16),
                pltpu.VMEM((4, half, n, slots, 2 * head), BF16),
                pltpu.VMEM((4, rows, head, seq), BF16),
                pltpu.VMEM((2, (heads + 3) * head, dim), BF16),
                pltpu.VMEM((2, heads * head, dim), BF16),
                pltpu.VMEM((2, experts, dim), BF16),
                pltpu.VMEM((2, hidden_rows, dim), BF16),
                pltpu.VMEM((2, hidden_rows, dim), BF16),
                pltpu.VMEM((2, hidden_rows, dim), BF16),
                pltpu.VMEM((5, rows, dim), BF16),
                pltpu.VMEM((2, dim), BF16),
                pltpu.VMEM((2, dim), BF16),
                pltpu.VMEM((2, top, rows), jnp.int32),
                pltpu.VMEM((8 * half, 2 * head), F32),
                pltpu.VMEM((half, 2 * head), F32),
                pltpu.VMEM((half, 2 * head), F32),
                pltpu.VMEM((8 * half, seq), F32),
                pltpu.VMEM((8 * half, seq), jnp.int32),
                pltpu.VMEM((rows, 2 * head), F32),
                pltpu.VMEM((rows, 2 * head), F32),
                pltpu.VMEM((chunks, 128, CHUNK), BF16),
                pltpu.VMEM((128, rows), F32),
                pltpu.VMEM((chunks, rows, CHUNK), BF16),
                pltpu.VMEM((4, rows, dim), BF16),
                pltpu.VMEM((4, n, half, dim // (n // 2)), BF16),
                dma((4,)), dma((5,)), dma((2, 5)), dma((2, chunks)), dma((2, chunks)), dma((2, chunks)),
                dma((4, 2, n)), dma((4, 2, n)), dma((4, n)), dma((4, n)), dma((4, n)), dma((4, n)), dma((4,)),
            ],
            compiler_params=pltpu.CompilerParams(
                collective_id=0, has_side_effects=True, vmem_limit_bytes=VMEM_BYTES),
            name='decode_two_layers',
        )(hidden, lengths, flip(choice), keys_one, vals_one, keys_two, vals_two, g_attn,
          flip(w_q), flip(w_k), flip(w_v), w_o, g_mlp, flip(w_router),
          flat(flip(w_gate)), flat(flip(w_up)), flat(w_down))
        outs = pl.pallas_call(
            pass_on,
            out_shape=[jax.ShapeDtypeStruct(o.shape, o.dtype) for o in outs],
            in_specs=[any_spec] * 5,
            out_specs=[any_spec] * 5,
            scratch_shapes=[pltpu.VMEM(o.shape, o.dtype) for o in outs] + [dma((5, 2)), dma((5, 2))],
            name='pass_on',
        )(*outs)
        back = lambda o: flip(o)[:, :, None, :]
        return (outs[0], back(outs[1]), back(outs[2]), back(outs[3]), back(outs[4]))

    return jax.shard_map(local_step, mesh=mesh, in_specs=(P('dp', None), P('dp'), P(None, 'dp', None), seq_spec, seq_spec, seq_spec, seq_spec, P(), col_spec, col_spec, col_spec, P(None, 'tp', None), P(), P(), ff_spec, ff_spec, P(None, None, 'tp', None)), out_specs=(P('dp', None), head_spec, head_spec, head_spec, head_spec), check_vma=False)
```
